32 devices in a mesh: groups: 2 (over y), ga: 16 (over z, x, core).
Axes of the slice: x: 2, y: 2, z: 4, core: 2. Of those that a mesh axis runs over, the one named last changes fastest.
Arguments:
- occupied: float32 [2, 1024, 12288], P(None, None, 'ga'), may hold values from -0.0546875 to 0.0546875
- residual: float32 [4, 2, 128, 12288], P('groups', None, None, 'ga'), parts along dimension 0, may hold values from -6 to 6
- old_direction: float32 [4, 2, 128, 12288], P('groups', None, None, 'ga'), parts along dimension 0, may hold values from -6 to 6
- kin_ratio: float32 [12288], P('ga'), may hold values from 0.06 to 5, as said below
- old_dot: float32 [4, 128], P('groups'), parts along dimension 0, may hold values from 6144 to 24576
Outputs:
- direction: float32 [4, 2, 128, 12288], P('groups', None, None, 'ga'), parts along dimension 0
- dot_new: float32 [4, 128], P('groups'), parts along dimension 0
The draws below stay inside these ranges and needn't reach their ends.
There are 2 independent parts, one for each index of `groups`. The reference program is written for one: setup_inputs(seed, part) draws one part's arguments, and reference() takes and returns one part's arrays. A program takes and returns all parts, laid end to end along the dimension named above; an argument that names none is the same for every part. Nothing has to cross between parts.
Inputs may be any that keep to these rules, and one draw needn't show every extreme that they name: `kin_ratio`: positive; grows with the plane-wave index on average and varies from one plane wave to the next.
All inputs are finite; a program needn't handle non-finite values.
Results may differ from the reference program's by a relative error of at most 0.000056.
Values sent between devices are 32-bit elements; how exact they have to be, the bound alone decides.
A program may use at most 64 MiB of HBM per device.

```python
import math
import jax
import jax.numpy as jnp
from jax import lax

NOCC = 1024
NB = 128
P_SIZE = 2
NG = 12288


def draw_kin_ratio(key, part):
    position = jnp.arange(NG, dtype=jnp.float32) / NG
    baseline = 0.1 + 3.0 * position ** (2.0 / 3.0)
    roughness = jnp.exp(jax.random.uniform(key, (NG,), jnp.float32, -0.4, 0.4))
    return baseline * roughness


def levels(stream_key, dims, shards, smallest, largest):
    factor_of = 1.0
    for dim, shards_of in shards:
        heights = jax.random.uniform(jax.random.fold_in(jax.random.fold_in(stream_key, 6), dim), (shards_of,), jnp.float32, smallest / len(shards), largest / len(shards))
        factor_of = factor_of * jnp.repeat(jnp.exp(heights), dims[dim] // shards_of).reshape((-1,) + (1,) * (len(dims) - 1 - dim))
    return factor_of


def bell_draw(own_key, shape, scale, most, split=(), kind=jnp.bfloat16):
    drawn = jax.random.normal(own_key, shape, jnp.float32) * scale
    if len(split) > 0:
        drawn = levels(own_key, shape, split, -0.22, 0.18) * drawn
    return jnp.clip(drawn, min=-most, max=most).astype(kind)


def setup_inputs(seed: int = 0, part: int = 0) -> dict:
    splits = jax.random.split(jax.random.key(seed), 6)
    own_keys = jax.random.split(jax.random.fold_in(splits[5], part), 6)
    return {
        "occupied": bell_draw(splits[0], (2, NOCC, NG), NG ** -0.5, 0.0546875, ((2, 16),), jnp.float32),
        "residual": bell_draw(own_keys[1], (P_SIZE, 2, NB, NG), 1.0, 6.0, ((3, 16),), jnp.float32),
        "old_direction": bell_draw(own_keys[2], (P_SIZE, 2, NB, NG), 1.0, 6.0, ((3, 16),), jnp.float32),
        "kin_ratio": draw_kin_ratio(jax.random.fold_in(splits[5], 71), part),
        "old_dot": jnp.clip(jnp.exp(jax.random.uniform(own_keys[4], (P_SIZE, NB), jnp.float32, math.log(6144.0), math.log(24576.0))), 6144.0, 24576.0),
    }


highest = lax.Precision.HIGHEST


def teter_factor(ratio):
    numerator = 27.0 + 18.0 * ratio + 12.0 * ratio ** 2 + 8.0 * ratio ** 3
    return numerator / (numerator + 16.0 * ratio ** 4)


def margins(occupied, vectors):
    products = jnp.einsum("hng,pcbg->phcnb", occupied, vectors, precision=highest)
    real_part = products[:, 0, 0] + products[:, 1, 1]
    imag_part = products[:, 0, 1] - products[:, 1, 0]
    return jnp.stack([real_part, imag_part], axis=1)


def correction(summed, occ_rows):
    real_part = summed[:, 0]
    imag_part = summed[:, 1]
    coefficient = jnp.stack([jnp.stack([real_part, -imag_part], axis=1), jnp.stack([imag_part, real_part], axis=1)], axis=1)
    return jnp.einsum("pchnb,hng->pcbg", coefficient, occ_rows, precision=highest)


def reference(occupied, residual, old_direction, kin_ratio, old_dot):
    factor = teter_factor(kin_ratio)
    first = margins(occupied, residual)
    gradient = residual - correction(first, occupied)
    precond = factor * gradient
    dot_new = jnp.sum(factor * (gradient[:, 0] ** 2 + gradient[:, 1] ** 2), axis=-1)
    second = margins(occupied, precond)
    projected = precond - correction(second, occupied)
    direction = projected + (dot_new / old_dot)[:, None, :, None] * old_direction
    return direction, dot_new
```

```python
import functools
import math

import jax
import jax.numpy as jnp
from jax import lax
from jax.experimental import pallas as pl
from jax.experimental.pallas import tpu as pltpu
from jax.sharding import PartitionSpec as P

HIGH = lax.Precision.HIGH


def teter_factor(ratio):
    numerator = 27.0 + 18.0 * ratio + 12.0 * ratio**2 + 8.0 * ratio**3
    return numerator / (numerator + 16.0 * ratio**4)


def levels_of(count):
    chips = count // 2
    inner = 2 ** (int(math.log2(chips)) // 2)
    return (2, inner, chips // inner)


def sum_kernel(levels, chunks, small, *refs):
    depth = len(levels)
    if small:
        x_ref, d_ref, o_ref, e_ref, *scratch = refs
        gathered = scratch[-depth:]
        scratch = scratch[:-depth]
    else:
        x_ref, o_ref, *scratch = refs
    recv = scratch[:depth]
    part = scratch[depth : 2 * depth - 1]
    send_sem, recv_sem = scratch[2 * depth - 1 :]
    me = lax.axis_index("ga")
    coords, strides, stride = [], [], 1
    for size in levels:
        coords.append((me // stride) % size)
        strides.append(stride)
        stride *= size
    rows = x_ref.shape[0] // chunks
    sizes = [rows]
    for size in levels:
        sizes.append(sizes[-1] // size)

    def peer(level, d):
        there = (coords[level] + d) % levels[level]
        return there, me + (there - coords[level]) * strides[level]

    barrier = pltpu.get_barrier_semaphore()
    total = 0
    for level in range(depth):
        for d in range(1, levels[level]):
            pl.semaphore_signal(barrier, inc=1, device_id={"ga": peer(level, d)[1]}, device_id_type=pl.DeviceIdType.MESH)
            total += 1
    pl.semaphore_wait(barrier, total)

    slot_of = {}

    def sem_slot(chunk, stage, d):
        return slot_of.setdefault((chunk, stage, d), len(slot_of))

    def own_start(chunk, level):
        start = chunk * rows
        for k in range(level):
            start = start + coords[k] * sizes[k + 1]
        return pl.multiple_of(start, 8)

    copies = {}

    def send(chunk, stage, d, src, dst, device):
        slot = sem_slot(chunk, stage, d)
        copy = pltpu.make_async_remote_copy(
            src_ref=src,
            dst_ref=dst,
            send_sem=send_sem.at[slot],
            recv_sem=recv_sem.at[slot],
            device_id={"ga": device},
            device_id_type=pl.DeviceIdType.MESH,
        )
        copy.start()
        copies[(chunk, stage, d)] = copy

    def source(chunk, level, which):
        height = sizes[level + 1]
        if level == 0:
            return x_ref.at[pl.ds(pl.multiple_of(chunk * rows + which * height, 8), height)]
        return part[level - 1].at[chunk, pl.ds(pl.multiple_of(which * height, 8), height)]

    def stage_run(chunk, stage):
        if 1 <= stage <= depth:
            level = stage - 1
            value = source(chunk, level, coords[level])[...]
            for d in range(1, levels[level]):
                copies[(chunk, stage - 1, d)].wait_recv()
                value = value + recv[level][chunk, d - 1]
            if level < depth - 1:
                part[level][chunk] = value
            else:
                o_ref[pl.ds(own_start(chunk, depth), sizes[depth])] = value
        elif stage > depth:
            level = 2 * depth - stage
            for d in range(1, levels[level]):
                copies[(chunk, stage - 1, d)].wait_recv()
        if stage < depth:
            for d in range(1, levels[stage]):
                there, device = peer(stage, d)
                send(chunk, stage, d, source(chunk, stage, there), recv[stage].at[chunk, d - 1], device)
        elif stage < 2 * depth:
            level = 2 * depth - 1 - stage
            block = o_ref.at[pl.ds(own_start(chunk, level + 1), sizes[level + 1])]
            for d in range(1, levels[level]):
                send(chunk, stage, d, block, block, peer(level, d)[1])

    def small_run(stage):
        if stage == 0:
            value = d_ref[...]
        else:
            for d in range(1, levels[stage - 1]):
                copies[("small", stage - 1, d)].wait_recv()
            value = gathered[stage - 1][0]
            for k in range(1, levels[stage - 1]):
                value = value + gathered[stage - 1][k]
        if stage == depth:
            e_ref[...] = value
            return
        gathered[stage][coords[stage]] = value
        block = gathered[stage].at[coords[stage]]
        for d in range(1, levels[stage]):
            send("small", stage, d, block, block, peer(stage, d)[1])

    for turn in range(chunks + 2 * depth):
        if small and turn <= depth:
            small_run(turn)
        for stage in reversed(range(2 * depth + 1)):
            chunk = turn - stage
            if 0 <= chunk < chunks:
                stage_run(chunk, stage)
    for copy in copies.values():
        copy.wait_send()


def sum_over_ga(x, count, ident, small=None):
    levels = levels_of(count)
    rows = x.shape[0]
    chunks = max(1, min(4, rows // (8 * count)))
    height = rows // chunks
    recv, part = [], []
    for level, size in enumerate(levels):
        height //= size
        recv.append(pltpu.VMEM((chunks, size - 1, height, x.shape[1]), x.dtype))
        if level < len(levels) - 1:
            part.append(pltpu.VMEM((chunks, height, x.shape[1]), x.dtype))
    slots = (2 * chunks + 1) * sum(size - 1 for size in levels)
    scratch = recv + part + [pltpu.SemaphoreType.DMA((slots,)), pltpu.SemaphoreType.DMA((slots,))]
    operands = [x]
    if small is not None:
        operands.append(small)
        scratch += [pltpu.VMEM((size,) + small.shape, small.dtype) for size in levels]
    return pl.pallas_call(
        functools.partial(sum_kernel, levels, chunks, small is not None),
        out_shape=[jax.ShapeDtypeStruct(a.shape, a.dtype) for a in operands],
        in_specs=[pl.BlockSpec(memory_space=pltpu.VMEM) for a in operands],
        out_specs=[pl.BlockSpec(memory_space=pltpu.VMEM) for a in operands],
        scratch_shapes=scratch,
        compiler_params=pltpu.CompilerParams(collective_id=ident, has_side_effects=True),
        name=f"sum_over_ga_{ident}",
    )(*operands)


def margins(occupied, vectors):
    turned = jnp.stack([vectors[:, 1], -vectors[:, 0]], axis=1)
    both = jnp.concatenate([vectors, turned], axis=2)
    return jnp.einsum("phmg,hng->pmn", both, occupied, precision=HIGH)


def correction(summed, occ_rows):
    half = summed.shape[1] // 2
    turned = jnp.concatenate([-summed[:, half:], summed[:, :half]], axis=1)
    coefficient = jnp.stack([summed, turned], axis=1)
    out = jnp.einsum("phmn,hng->pmg", coefficient, occ_rows, precision=HIGH)
    return out.reshape(out.shape[0], 2, half, out.shape[2])


def on_device(count, occupied, residual, old_direction, kin_ratio, old_dot):
    pert, _, bands, _ = residual.shape
    occ = occupied.shape[1]
    factor = teter_factor(kin_ratio)

    shape = (pert, 2 * bands, occ)
    lanes = occ if pert * 2 * bands % (8 * count) == 0 else 128

    def to_rows(s):
        return s.reshape(-1, lanes)

    def from_rows(r):
        return r.reshape(shape)

    first = from_rows(sum_over_ga(to_rows(margins(occupied, residual)), count, 0)[0])
    gradient = residual - correction(first, occupied)
    precond = factor * gradient
    local_dot = jnp.sum(factor * (gradient[:, 0] ** 2 + gradient[:, 1] ** 2), axis=-1)
    padded = jnp.pad(local_dot, ((0, -pert % 8), (0, 0)))
    second, dots = sum_over_ga(to_rows(margins(occupied, precond)), count, 1, padded)
    second = from_rows(second)
    dot_new = dots[:pert]
    projected = precond - correction(second, occupied)
    direction = projected + (dot_new / old_dot)[:, None, :, None] * old_direction
    return (direction, dot_new)


def solution(mesh):
    placed = (
        P(None, None, "ga"),
        P("groups", None, None, "ga"),
        P("groups", None, None, "ga"),
        P("ga"),
        P("groups", None),
    )
    return jax.shard_map(
        functools.partial(on_device, mesh.shape["ga"]),
        mesh=mesh,
        in_specs=placed,
        out_specs=(P("groups", None, None, "ga"), P("groups", None)),
        check_vma=False,
    )
```

```python
import functools
import math

import jax
import jax.numpy as jnp
from jax import lax
from jax.experimental import pallas as pl
from jax.experimental.pallas import tpu as pltpu
from jax.sharding import PartitionSpec as P


def teter_factor(ratio):
    numerator = 27.0 + 18.0 * ratio + 12.0 * ratio**2 + 8.0 * ratio**3
    return numerator / (numerator + 16.0 * ratio**4)


def levels_of(count):
    chips = count // 2
    inner = 2 ** (int(math.log2(chips)) // 2)
    return (2, inner, chips // inner)


def plan_of(levels, rows, lanes):
    cuts = []
    for size in levels:
        if rows % (8 * size) == 0:
            rows //= size
            cuts.append((0, rows, lanes))
        elif lanes % (128 * size) == 0:
            lanes //= size
            cuts.append((1, rows, lanes))
        else:
            return None
    return cuts


def split(x):
    high = x.astype(jnp.bfloat16)
    return high, (x - high.astype(jnp.float32)).astype(jnp.bfloat16)


def three_pass(a, b, dims):
    def dot(u, v):
        return lax.dot_general(u, v, (dims, ((), ())), preferred_element_type=jnp.float32)

    return dot(a[0], b[0]) + (dot(a[0], b[1]) + dot(a[1], b[0]))


def project_kernel(levels, cuts, pieces, small, *refs):
    depth = len(levels)
    if small:
        r_ref, occ_ref, d_ref, c_ref, e_ref, *scratch = refs
        gathered = scratch[-depth:]
        scratch = scratch[:-depth]
    else:
        r_ref, occ_ref, c_ref, *scratch = refs
    local, total, occ_high, occ_low, r_high, r_low, *scratch = scratch
    recv = scratch[:depth]
    part = scratch[depth : 2 * depth - 1]
    send_sem, recv_sem = scratch[2 * depth - 1 :]
    pert, rows, _ = r_ref.shape
    half = rows // 2
    width = occ_ref.shape[1] // pieces
    chunks = pert * pieces
    me = lax.axis_index("ga")
    coords, strides, stride = [], [], 1
    for size in levels:
        coords.append((me // stride) % size)
        strides.append(stride)
        stride *= size

    def peer(level, d):
        there = (coords[level] + d) % levels[level]
        return there, me + (there - coords[level]) * strides[level]

    barrier = pltpu.get_barrier_semaphore()
    count = 0
    for level in range(depth):
        for d in range(1, levels[level]):
            pl.semaphore_signal(barrier, inc=1, device_id={"ga": peer(level, d)[1]}, device_id_type=pl.DeviceIdType.MESH)
            count += 1

    copies = {}

    def send(chunk, stage, d, src, dst, device):
        slot = len(copies)
        copy = pltpu.make_async_remote_copy(
            src_ref=src,
            dst_ref=dst,
            send_sem=send_sem.at[slot],
            recv_sem=recv_sem.at[slot],
            device_id={"ga": device},
            device_id_type=pl.DeviceIdType.MESH,
        )
        copy.start()
        copies[(chunk, stage, d)] = copy

    def band(chunk):
        p, q = divmod(chunk, pieces)
        return p, q * width

    def inside(level, which, row, lane):
        axis, height, span = cuts[level]
        if axis == 0:
            return row + which * height, lane
        return row, lane + which * span

    def window(chunk, level, row, lane):
        _, height, span = cuts[level]
        return pl.ds(pl.multiple_of(row, 8), height), pl.ds(pl.multiple_of(lane, 128), span)

    def owned(chunk, level):
        p, lane = band(chunk)
        row = 0
        for k in range(level + 1):
            row, lane = inside(k, coords[k], row, lane)
        return total.at[(p,) + window(chunk, level, row, lane)]

    def source(chunk, level, which):
        if level == 0:
            p, lane = band(chunk)
            return local.at[(p,) + window(chunk, 0, *inside(0, which, 0, lane))]
        return part[level - 1].at[(chunk,) + window(chunk, level, *inside(level, which, 0, 0))]

    def form(chunk):
        p, lane = band(chunk)
        bands = pl.ds(lane, width)
        if p == 0:
            for h in range(2):
                occ_high[h, bands], occ_low[h, bands] = split(occ_ref[h, bands])
        if lane == 0:
            r_high[p], r_low[p] = split(r_ref[p])
        vectors = (r_high[p], r_low[p])
        first, second = (three_pass(vectors, (occ_high[h, bands], occ_low[h, bands]), ((1,), (1,))) for h in range(2))
        local[p, :half, bands] = first[:half] + second[half:]
        local[p, half:, bands] = first[half:] - second[:half]

    def correct(chunk):
        p, lane = band(chunk)
        bands = pl.ds(lane, width)
        summed = split(total[p, :, bands])
        first, second = (three_pass(summed, (occ_high[h, bands], occ_low[h, bands]), ((1,), (0,))) for h in range(2))
        upper = first[:half] - second[half:]
        lower = first[half:] + second[:half]
        if lane == 0:
            c_ref[p, :half] = upper
            c_ref[p, half:] = lower
        else:
            c_ref[p, :half] += upper
            c_ref[p, half:] += lower

    def stage_run(chunk, stage):
        if 1 <= stage <= depth:
            level = stage - 1
            value = source(chunk, level, coords[level])[...]
            for d in range(1, levels[level]):
                copies[(chunk, stage - 1, d)].wait_recv()
                value = value + recv[level][chunk, d - 1]
            if level < depth - 1:
                part[level][chunk] = value
            else:
                owned(chunk, depth - 1)[...] = value
        elif stage > depth:
            level = 2 * depth - stage
            for d in range(1, levels[level]):
                copies[(chunk, stage - 1, d)].wait_recv()
        if stage < depth:
            for d in range(1, levels[stage]):
                there, device = peer(stage, d)
                send(chunk, stage, d, source(chunk, stage, there), recv[stage].at[chunk, d - 1], device)
        elif stage < 2 * depth:
            level = 2 * depth - 1 - stage
            block = owned(chunk, level)
            for d in range(1, levels[level]):
                send(chunk, stage, d, block, block, peer(level, d)[1])
        else:
            correct(chunk)

    def small_run(stage):
        if stage == 0:
            value = d_ref[...]
        else:
            for d in range(1, levels[stage - 1]):
                copies[("small", stage - 1, d)].wait_recv()
            value = gathered[stage - 1][0]
            for k in range(1, levels[stage - 1]):
                value = value + gathered[stage - 1][k]
        if stage == depth:
            e_ref[...] = value
            return
        gathered[stage][coords[stage]] = value
        block = gathered[stage].at[coords[stage]]
        for d in range(1, levels[stage]):
            send("small", stage, d, block, block, peer(stage, d)[1])

    order = [0] + list(reversed(range(1, 2 * depth))) + [2 * depth]
    for turn in range(chunks + 2 * depth):
        for stage in order:
            chunk = turn - stage
            if 0 <= chunk < chunks:
                if stage == 0:
                    form(chunk)
                    if chunk == 0:
                        pl.semaphore_wait(barrier, count)
                stage_run(chunk, stage)
        if small and turn <= depth:
            small_run(turn)
    for copy in copies.values():
        copy.wait_send()


def project(vectors, occupied, count, ident, small=None):
    levels = levels_of(count)
    pert, rows, planes = vectors.shape
    occ = occupied.shape[1]
    for pieces in (4, 2, 1):
        cuts = plan_of(levels, rows, occ // pieces)
        if cuts is not None:
            break
    chunks = pert * pieces
    recv, part = [], []
    for level, size in enumerate(levels):
        shape = cuts[level][1:]
        recv.append(pltpu.VMEM((chunks, size - 1) + shape, jnp.float32))
        if level < len(levels) - 1:
            part.append(pltpu.VMEM((chunks,) + shape, jnp.float32))
    slots = (2 * chunks + 1) * sum(size - 1 for size in levels)
    scratch = [pltpu.VMEM((pert, rows, occ), jnp.float32)] * 2
    scratch += [pltpu.VMEM(occupied.shape, jnp.bfloat16)] * 2 + [pltpu.VMEM(vectors.shape, jnp.bfloat16)] * 2
    scratch += recv + part + [pltpu.SemaphoreType.DMA((slots,)), pltpu.SemaphoreType.DMA((slots,))]
    operands = [vectors, occupied]
    outs = [jax.ShapeDtypeStruct(vectors.shape, vectors.dtype)]
    if small is not None:
        operands.append(small)
        outs.append(jax.ShapeDtypeStruct(small.shape, small.dtype))
        scratch += [pltpu.VMEM((size,) + small.shape, small.dtype) for size in levels]
    return pl.pallas_call(
        functools.partial(project_kernel, levels, cuts, pieces, small is not None),
        out_shape=outs,
        in_specs=[pl.BlockSpec(memory_space=pltpu.VMEM) for _ in operands],
        out_specs=[pl.BlockSpec(memory_space=pltpu.VMEM) for _ in outs],
        scratch_shapes=scratch,
        compiler_params=pltpu.CompilerParams(collective_id=ident, has_side_effects=True),
        name=f"project_{ident}",
    )(*operands)


def on_device(count, occupied, residual, old_direction, kin_ratio, old_dot):
    pert, _, bands, planes = residual.shape
    flat = (pert, 2 * bands, planes)
    factor = teter_factor(kin_ratio)
    (first,) = project(residual.reshape(flat), occupied, count, 0)
    gradient = residual - first.reshape(residual.shape)
    precond = factor * gradient
    local_dot = jnp.sum(factor * (gradient[:, 0] ** 2 + gradient[:, 1] ** 2), axis=-1)
    padded = jnp.pad(local_dot, ((0, -pert % 8), (0, 0)))
    second, dots = project(precond.reshape(flat), occupied, count, 1, padded)
    dot_new = dots[:pert]
    projected = precond - second.reshape(residual.shape)
    direction = projected + (dot_new / old_dot)[:, None, :, None] * old_direction
    return (direction, dot_new)


def solution(mesh):
    placed = (
        P(None, None, "ga"),
        P("groups", None, None, "ga"),
        P("groups", None, None, "ga"),
        P("ga"),
        P("groups", None),
    )
    return jax.shard_map(
        functools.partial(on_device, mesh.shape["ga"]),
        mesh=mesh,
        in_specs=placed,
        out_specs=(P("groups", None, None, "ga"), P("groups", None)),
        check_vma=False,
    )
```

```python
import functools
import math

import jax
import jax.numpy as jnp
from jax import lax
from jax.experimental import pallas as pl
from jax.experimental.pallas import tpu as pltpu
from jax.sharding import PartitionSpec as P


def teter_factor(ratio):
    numerator = 27.0 + 18.0 * ratio + 12.0 * ratio**2 + 8.0 * ratio**3
    return numerator / (numerator + 16.0 * ratio**4)


def levels_of(count):
    chips = count // 2
    inner = 2 ** (int(math.log2(chips)) // 2)
    return (2, inner, chips // inner)


def plan_of(levels, rows, lanes):
    cuts = []
    for size in levels:
        if rows % (8 * size) == 0:
            rows //= size
            cuts.append((0, rows, lanes))
        elif lanes % (128 * size) == 0:
            lanes //= size
            cuts.append((1, rows, lanes))
        else:
            return None
    return cuts


def split(x):
    high = x.astype(jnp.bfloat16)
    return high, (x - high.astype(jnp.float32)).astype(jnp.bfloat16)


def three_pass(a, b, dims):
    def dot(u, v):
        return lax.dot_general(u, v, (dims, ((), ())), preferred_element_type=jnp.float32)

    return dot(a[0], b[0]) + (dot(a[0], b[1]) + dot(a[1], b[0]))


def project_kernel(levels, cuts, pieces, small, *refs):
    depth = len(levels)
    if small:
        r_ref, occ_ref, d_ref, c_ref, e_ref, *scratch = refs
        gathered = scratch[-depth:]
        scratch = scratch[:-depth]
    else:
        r_ref, occ_ref, c_ref, *scratch = refs
    local, total, occ_high, occ_low, r_high, r_low, *scratch = scratch
    recv = scratch[:depth]
    part = scratch[depth : 2 * depth - 1]
    send_sem, recv_sem = scratch[2 * depth - 1 :]
    pert, rows, _ = r_ref.shape
    half = rows // 2
    width = occ_ref.shape[1] // pieces
    chunks = pert * pieces
    me = lax.axis_index("ga")
    coords, strides, stride = [], [], 1
    for size in levels:
        coords.append((me // stride) % size)
        strides.append(stride)
        stride *= size

    def peer(level, d):
        there = (coords[level] + d) % levels[level]
        return there, me + (there - coords[level]) * strides[level]

    barrier = pltpu.get_barrier_semaphore()
    count = 0
    for level in range(depth):
        for d in range(1, levels[level]):
            pl.semaphore_signal(barrier, inc=1, device_id={"ga": peer(level, d)[1]}, device_id_type=pl.DeviceIdType.MESH)
            count += 1

    copies = {}

    def send(chunk, stage, d, src, dst, device):
        slot = len(copies)
        copy = pltpu.make_async_remote_copy(
            src_ref=src,
            dst_ref=dst,
            send_sem=send_sem.at[slot],
            recv_sem=recv_sem.at[slot],
            device_id={"ga": device},
            device_id_type=pl.DeviceIdType.MESH,
        )
        copy.start()
        copies[(chunk, stage, d)] = copy

    def band(chunk):
        p, q = divmod(chunk, pieces)
        return p, q * width

    def inside(level, which, row, lane):
        axis, height, span = cuts[level]
        if axis == 0:
            return row + which * height, lane
        return row, lane + which * span

    def window(chunk, level, row, lane):
        _, height, span = cuts[level]
        return pl.ds(pl.multiple_of(row, 8), height), pl.ds(pl.multiple_of(lane, 128), span)

    def owned(chunk, level):
        p, lane = band(chunk)
        row = 0
        for k in range(level + 1):
            row, lane = inside(k, coords[k], row, lane)
        return total.at[(p,) + window(chunk, level, row, lane)]

    def source(chunk, level, which):
        if level == 0:
            p, lane = band(chunk)
            return local.at[(p,) + window(chunk, 0, *inside(0, which, 0, lane))]
        return part[level - 1].at[(chunk,) + window(chunk, level, *inside(level, which, 0, 0))]

    def form(chunk):
        p, lane = band(chunk)
        bands = pl.ds(lane, width)
        if p == 0:
            for h in range(2):
                occ_high[h, bands], occ_low[h, bands] = split(occ_ref[h, bands])
        if lane == 0:
            r_high[p], r_low[p] = split(r_ref[p])
        vectors = (r_high[p], r_low[p])
        first, second = (three_pass(vectors, (occ_high[h, bands], occ_low[h, bands]), ((1,), (1,))) for h in range(2))
        local[p, :half, bands] = first[:half] + second[half:]
        local[p, half:, bands] = first[half:] - second[:half]

    def correct(chunk):
        p, lane = band(chunk)
        bands = pl.ds(lane, width)
        summed = split(total[p, :, bands])
        first, second = (three_pass(summed, (occ_high[h, bands], occ_low[h, bands]), ((1,), (0,))) for h in range(2))
        upper = first[:half] - second[half:]
        lower = first[half:] + second[:half]
        if lane == 0:
            c_ref[p, :half] = upper
            c_ref[p, half:] = lower
        else:
            c_ref[p, :half] += upper
            c_ref[p, half:] += lower

    def stage_run(chunk, stage):
        if 1 <= stage <= depth:
            level = stage - 1
            value = source(chunk, level, coords[level])[...]
            for d in range(1, levels[level]):
                copies[(chunk, stage - 1, d)].wait_recv()
                value = value + recv[level][chunk, d - 1]
            if level < depth - 1:
                part[level][chunk] = value
            else:
                owned(chunk, depth - 1)[...] = value
        elif stage > depth:
            level = 2 * depth - stage
            for d in range(1, levels[level]):
                copies[(chunk, stage - 1, d)].wait_recv()
        if stage < depth:
            for d in range(1, levels[stage]):
                there, device = peer(stage, d)
                send(chunk, stage, d, source(chunk, stage, there), recv[stage].at[chunk, d - 1], device)
        elif stage < 2 * depth:
            level = 2 * depth - 1 - stage
            block = owned(chunk, level)
            for d in range(1, levels[level]):
                send(chunk, stage, d, block, block, peer(level, d)[1])
        else:
            correct(chunk)

    def small_run(stage):
        if stage == 0:
            value = d_ref[...]
        else:
            for d in range(1, levels[stage - 1]):
                copies[("small", stage - 1, d)].wait_recv()
            value = gathered[stage - 1][0]
            for k in range(1, levels[stage - 1]):
                value = value + gathered[stage - 1][k]
        if stage == depth:
            e_ref[...] = value
            return
        gathered[stage][coords[stage]] = value
        block = gathered[stage].at[coords[stage]]
        for d in range(1, levels[stage]):
            send("small", stage, d, block, block, peer(stage, d)[1])

    order = [0] + list(reversed(range(1, 2 * depth))) + [2 * depth]
    for turn in range(chunks + 2 * depth):
        for stage in order:
            chunk = turn - stage
            if 0 <= chunk < chunks:
                if stage == 0:
                    form(chunk)
                    if chunk == 0:
                        pl.semaphore_wait(barrier, count)
                stage_run(chunk, stage)
        if small and turn <= depth:
            small_run(turn)
    for copy in copies.values():
        copy.wait_send()


def project(vectors, occupied, count, ident, small=None):
    levels = levels_of(count)
    pert, rows, planes = vectors.shape
    occ = occupied.shape[1]
    for pieces in (2, 1):
        cuts = plan_of(levels, rows, occ // pieces)
        if cuts is not None:
            break
    chunks = pert * pieces
    recv, part = [], []
    for level, size in enumerate(levels):
        shape = cuts[level][1:]
        recv.append(pltpu.VMEM((chunks, size - 1) + shape, jnp.float32))
        if level < len(levels) - 1:
            part.append(pltpu.VMEM((chunks,) + shape, jnp.float32))
    slots = (2 * chunks + 1) * sum(size - 1 for size in levels)
    scratch = [pltpu.VMEM((pert, rows, occ), jnp.float32)] * 2
    scratch += [pltpu.VMEM(occupied.shape, jnp.bfloat16)] * 2 + [pltpu.VMEM(vectors.shape, jnp.bfloat16)] * 2
    scratch += recv + part + [pltpu.SemaphoreType.DMA((slots,)), pltpu.SemaphoreType.DMA((slots,))]
    operands = [vectors, occupied]
    outs = [jax.ShapeDtypeStruct(vectors.shape, vectors.dtype)]
    if small is not None:
        operands.append(small)
        outs.append(jax.ShapeDtypeStruct(small.shape, small.dtype))
        scratch += [pltpu.VMEM((size,) + small.shape, small.dtype) for size in levels]
    return pl.pallas_call(
        functools.partial(project_kernel, levels, cuts, pieces, small is not None),
        out_shape=outs,
        in_specs=[pl.BlockSpec(memory_space=pltpu.VMEM) for _ in operands],
        out_specs=[pl.BlockSpec(memory_space=pltpu.VMEM) for _ in outs],
        scratch_shapes=scratch,
        compiler_params=pltpu.CompilerParams(collective_id=ident, has_side_effects=True),
        name=f"project_{ident}",
    )(*operands)


def on_device(count, occupied, residual, old_direction, kin_ratio, old_dot):
    pert, _, bands, planes = residual.shape
    flat = (pert, 2 * bands, planes)
    factor = teter_factor(kin_ratio)
    (first,) = project(residual.reshape(flat), occupied, count, 0)
    gradient = residual - first.reshape(residual.shape)
    precond = factor * gradient
    local_dot = jnp.sum(factor * (gradient[:, 0] ** 2 + gradient[:, 1] ** 2), axis=-1)
    padded = jnp.pad(local_dot, ((0, -pert % 8), (0, 0)))
    second, dots = project(precond.reshape(flat), occupied, count, 1, padded)
    dot_new = dots[:pert]
    projected = precond - second.reshape(residual.shape)
    direction = projected + (dot_new / old_dot)[:, None, :, None] * old_direction
    return (direction, dot_new)


def solution(mesh):
    placed = (
        P(None, None, "ga"),
        P("groups", None, None, "ga"),
        P("groups", None, None, "ga"),
        P("ga"),
        P("groups", None),
    )
    return jax.shard_map(
        functools.partial(on_device, mesh.shape["ga"]),
        mesh=mesh,
        in_specs=placed,
        out_specs=(P("groups", None, None, "ga"), P("groups", None)),
        check_vma=False,
    )
```
